512 devices in a mesh: dp: 2 (over core), seq: 8 (over z), vocab: 32 (over y, x).
Axes of the slice: x: 4, y: 8, z: 8, core: 2. Of those that a mesh axis runs over, the one named last changes fastest.
Arguments:
- hidden_states: bfloat16 [6, 1024, 4096], P('dp', 'seq', 'vocab'), may hold values from -6 to 6
- head_weight: bfloat16 [4096, 32000], P('seq', 'vocab'), may hold values from -0.09375 to 0.09375
- owner_pos: int32 [6, 32000], P('dp', 'vocab'), may hold values from 0 to 1023
- token_ids: int32 [6, 1024], P('dp', 'seq'), may hold values from 0 to 31999, as said below
- teacher_margin: float32 [2], P('dp'), may hold values from -150 to 150
Outputs:
- grad_head: float32 [4096, 32000], P('seq', 'vocab')
- grad_hidden: bfloat16 [6, 1024, 4096], P('dp', 'seq', 'vocab')
The draws below stay inside these ranges and needn't reach their ends.
Inputs may be any that keep to these rules, and one draw needn't show every extreme that they name: `owner_pos`: owner positions may fall on padding tokens, which then pool nothing. `token_ids`: 0 marks padding, which fills a tail of one or more positions of every document; a document's first token is 31999.
All inputs are finite; a program needn't handle non-finite values.
Results may differ from the reference program's by a relative error of at most 0.017.
Values may be sent and summed in bfloat16 or wider, within the bound.
A program may use at most 64 MiB of HBM per device.

```python
import jax
import jax.numpy as jnp
from jax import lax

D = 4096
VOCAB = 32000
TRIPLES = 2
DOCS = 6
L = 1024
N_VOCAB = 32


def draw_token_ids(key, part):
    key_length, key_values = jax.random.split(key)
    lengths = jax.random.randint(key_length, (DOCS, 1), L // 2, L)
    values = jax.random.randint(key_values, (DOCS, L), 1, VOCAB)
    positions = jnp.arange(L, dtype=jnp.int32)[None, :]
    values = jnp.where(positions < lengths, values, 0)
    values = values.at[:, 0].set(VOCAB - 1)
    return values.astype(jnp.int32)


def plant(values, stream_key, least, top_value):
    extent = values.shape
    place = [jax.random.randint(jax.random.fold_in(stream_key, axis), (), 0, extent[axis]) for axis in range(len(extent))]
    values = values.at[tuple(place)].set(least)
    longest = extent.index(max(extent))
    place[longest] = (place[longest] + 1) % extent[longest]
    return values.at[tuple(place)].set(top_value)


def shard_levels(stream_key, dims, cuts, low, high):
    factor_of, own = 1.0, jax.random.fold_in(stream_key, 6)
    for position, parts in cuts:
        draws = jnp.exp(jax.random.uniform(jax.random.fold_in(own, position), (parts,), jnp.float32, low / len(cuts), high / len(cuts)))
        factor_of = factor_of * jnp.repeat(draws, dims[position] // parts).reshape([-1 if axis == position else 1 for axis in range(len(dims))])
    return factor_of


def scatter_about(key, dims, width, limit, cuts=(), kind=jnp.bfloat16):
    level = shard_levels(key, dims, cuts, -0.22, 0.18) if cuts else 1.0
    result = jax.random.normal(key, dims, jnp.float32) * width * level
    return jnp.minimum(jnp.maximum(result, -limit), limit).astype(kind)


def setup_inputs(seed: int = 0) -> dict:
    arg_keys = jax.random.split(jax.random.key(seed), 6)
    return {
        "hidden_states": scatter_about(arg_keys[0], (DOCS, L, D), 1.0, 6.0, ((0, 2), (1, 8), (2, 32))),
        "head_weight": scatter_about(arg_keys[1], (D, VOCAB), D ** -0.5, 0.09375, ((0, 8), (1, 32))),
        "owner_pos": plant(jax.random.randint(arg_keys[2], (DOCS, VOCAB), 0, L), jax.random.fold_in(arg_keys[2], 1), 0, L - 1).astype(jnp.int32),
        "token_ids": draw_token_ids(jax.random.fold_in(arg_keys[5], 71), 0),
        "teacher_margin": scatter_about(arg_keys[4], (TRIPLES,), 30.0, 150.0, ((0, 2),), jnp.float32),
    }


def pick_rows(features, places):
    return features[places]

def reference(hidden_states, head_weight, owner_pos, token_ids, teacher_margin):
    block_count = N_VOCAB
    block_size = VOCAB // block_count
    head_blocks = head_weight.T.reshape(block_count, block_size, D)

    def doc_logits(inputs):
        features, places = inputs

        def block_logits(pair):
            block_places, block_head = pair
            owner_rows = pick_rows(features, block_places).astype(jnp.float32)
            return lax.optimization_barrier(jnp.sum(owner_rows * block_head.astype(jnp.float32), axis=1))
        return lax.map(block_logits, (places.reshape(block_count, block_size), head_blocks)).reshape(VOCAB)
    logits = lax.map(doc_logits, (hidden_states, owner_pos))
    validity = (jnp.take_along_axis(token_ids, owner_pos, axis=1) != 0).astype(jnp.float32)
    softened = jax.nn.softplus(logits)
    pooled = validity * jnp.log1p(softened)
    slopes = validity * jax.nn.sigmoid(logits) / (1.0 + softened)
    triple_view = pooled.reshape(TRIPLES, 3, VOCAB)
    positive = lax.optimization_barrier(jnp.sum(triple_view[:, 0] * triple_view[:, 1], axis=1))
    negative = lax.optimization_barrier(jnp.sum(triple_view[:, 0] * triple_view[:, 2], axis=1))
    margin_grad = (positive - negative - teacher_margin) / TRIPLES
    scale = margin_grad[:, None]
    pooled_grad = jnp.stack([scale * (triple_view[:, 1] - triple_view[:, 2]), scale * triple_view[:, 0], -scale * triple_view[:, 0]], axis=1).reshape(DOCS, VOCAB)
    grad_logit = (pooled_grad * slopes).astype(jnp.bfloat16)

    def head_block(inputs):
        block_places, block_grads = inputs
        owner_rows = jax.vmap(pick_rows)(hidden_states, block_places).astype(jnp.float32)
        return jnp.einsum('kvd,kv->dv', owner_rows, block_grads.astype(jnp.float32), precision=lax.Precision.HIGHEST)
    places_blocks = owner_pos.reshape(DOCS, block_count, block_size).transpose(1, 0, 2)
    grads_blocks = grad_logit.reshape(DOCS, block_count, block_size).transpose(1, 0, 2)
    head_parts = lax.map(head_block, (places_blocks, grads_blocks))
    grad_head = head_parts.transpose(1, 0, 2).reshape(D, VOCAB)

    def doc_grad(inputs):
        places, grads = inputs

        def advance(running, block):
            block_places, block_grads, block_head = block
            products = block_grads.astype(jnp.float32)[:, None] * block_head.astype(jnp.float32)
            partial_value = jax.ops.segment_sum(products, block_places, num_segments=L)
            rounded = lax.optimization_barrier(partial_value.astype(jnp.bfloat16))
            return (running + rounded.astype(jnp.float32), None)
        running, _ = lax.scan(advance, jnp.zeros((L, D), jnp.float32), (places.reshape(block_count, block_size), grads.reshape(block_count, block_size), head_blocks))
        return running.astype(jnp.bfloat16)
    grad_hidden = lax.map(doc_grad, (owner_pos, grad_logit))
    return (grad_head, grad_hidden)
```

```python
import functools

import jax
import jax.numpy as jnp
from jax import lax
from jax.experimental import pallas as pl
from jax.experimental.pallas import tpu as pltpu
from jax.sharding import PartitionSpec as P

MESH = pl.DeviceIdType.MESH
F32 = jnp.float32
BF16 = jnp.bfloat16
NX, NY, NZ, NC = 4, 8, 8, 2
DOCS = 3
LO, HI = 256, 4
FEATS = 128
TERMS = 1000
WIDE = 1024
PIECE = 16


def kernel(
    scale, hid, w, own, tok, teacher, gh_out, gx_out,
    wall, oall, hall, ht, rows, lpart, lrecv, zbuf, ubuf, ybuf, pacc, pk, precv, ghb, ghr, ghx, fin,
    w_s, w_r, o_s, o_r, s1_s, s1_r, h_s, h_r, l_s, l_r, z_s, z_r, u_s, u_r, y_s, y_r,
    p_s, p_r, c_s, c_r, g_s, g_r, f_s, f_r, loc,
):
    c = lax.axis_index("dp")
    z = lax.axis_index("seq")
    v = lax.axis_index("vocab")
    y, x = v // NX, lax.rem(v, NX)

    def dev(cc, zz, yy, xx):
        return (cc, zz, yy * NX + xx)

    def turn(i, o, n):
        return lax.rem(i + o, n)

    def remote(src, dst, ss, rs, to):
        return pltpu.make_async_remote_copy(
            src_ref=src, dst_ref=dst, send_sem=ss, recv_sem=rs, device_id=to, device_id_type=MESH
        )

    me = dev(c, z, y, x)
    diagonal = y == z

    def x_copy(src, dst, ss, rs, o):
        to = dev(c, z, y, turn(x, o, NX))
        return remote(src, dst, ss.at[o], rs.at[NX - o], to)

    def scatter_copy(o):
        j = turn(y, o, NY)
        src = hid.at[:, pl.ds(pl.multiple_of(PIECE * j, PIECE), PIECE), :]
        dst = hall.at[:, j, pl.ds(pl.multiple_of(PIECE * z, PIECE), PIECE), :]
        slot = lax.rem(z - y + NZ, NZ)
        return remote(src, dst, s1_s.at[o], s1_r.at[slot], dev(c, y, j, x))

    def scatter_local():
        src = hid.at[:, pl.ds(pl.multiple_of(PIECE * y, PIECE), PIECE), :]
        dst = hall.at[:, y, pl.ds(pl.multiple_of(PIECE * z, PIECE), PIECE), :]
        return pltpu.make_async_copy(src, dst, loc.at[0])

    def spread_copy(k, o):
        block = hall.at[k, y]
        return remote(block, block, h_s.at[k, o], h_r.at[k, NY - o], dev(c, z, turn(y, o, NY), x))

    def return_copy(o):
        zz = turn(z, o, NZ)
        src = fin.at[:, pl.ds(pl.multiple_of(PIECE * zz, PIECE), PIECE), :]
        dst = gx_out.at[:, pl.ds(pl.multiple_of(PIECE * y, PIECE), PIECE), :]
        slot = lax.rem(y - z + NY, NY)
        return remote(src, dst, f_s.at[o], f_r.at[slot], dev(c, zz, z, x))

    def return_local():
        src = fin.at[:, pl.ds(pl.multiple_of(PIECE * z, PIECE), PIECE), :]
        dst = gx_out.at[:, pl.ds(pl.multiple_of(PIECE * y, PIECE), PIECE), :]
        return pltpu.make_async_copy(src, dst, loc.at[1])

    barrier = pltpu.get_barrier_semaphore()

    def greet(to):
        pl.semaphore_signal(barrier, inc=1, device_id=to, device_id_type=MESH)

    for o in range(NY):
        greet(dev(c, y, turn(y, o, NY), x))
        greet(dev(c, turn(z, o, NZ), z, x))
    for o in range(1, NY):
        greet(dev(c, z, turn(y, o, NY), x))
        greet(dev(c, turn(z, o, NZ), y, x))
    for o in range(1, NX):
        greet(dev(c, z, y, turn(x, o, NX)))
        greet(dev(1 - c, z, y, turn(x, o, NX)))
    greet(dev(1 - c, z, y, x))

    wall[x] = w[pl.ds(pl.multiple_of(x * FEATS, FEATS), FEATS), :]
    oall[x] = own[...]
    lpart[...] = jnp.zeros_like(lpart)
    count = jnp.sum((tok[...] != 0).astype(F32), axis=1, keepdims=True)
    pl.semaphore_wait(barrier, 2 * NY + 2 * (NY - 1) + 2 * (NX - 1) + 1)

    @pl.when(diagonal)
    def _():
        scatter_local().start()

    @pl.when(jnp.logical_not(diagonal))
    def _():
        scatter_copy(0).start()

    for o in range(1, NY):
        scatter_copy(o).start()
    for o in range(1, NX):
        x_copy(own, oall.at[x], o_s, o_r, o).start()
    for o in range(1, NX):
        i = turn(x, o, NX)
        src = w.at[pl.ds(pl.multiple_of(i * FEATS, FEATS), FEATS), :]
        x_copy(src, wall.at[x], w_s, w_r, o).start()

    @pl.when(diagonal)
    def _():
        scatter_local().wait()

    @pl.when(jnp.logical_not(diagonal))
    def _():
        scatter_copy(0).wait_send()
        remote(hid.at[:, pl.ds(0, PIECE), :], hall.at[:, y, pl.ds(0, PIECE), :], s1_s.at[0], s1_r.at[0], me).wait_recv()

    for o in range(1, NY):
        remote(hid.at[:, pl.ds(0, PIECE), :], hall.at[:, y, pl.ds(0, PIECE), :], s1_s.at[o], s1_r.at[o], me).wait_recv()
    for k in range(DOCS):
        for o in range(1, NY):
            spread_copy(k, o).start()

    for o in range(1, NX):
        i = turn(x, o, NX)
        remote(own, oall.at[i], o_s.at[o], o_r.at[o], me).wait_recv()
        remote(w.at[pl.ds(0, FEATS), :], wall.at[i], w_s.at[o], w_r.at[o], me).wait_recv()

    def split(owner):
        low = ((owner >> 4) & 1) * 128 + (owner >> 7) * PIECE + (owner & (PIECE - 1))
        return low, (owner >> 5) & 3

    for k in range(DOCS):
        for o in range(1, NY):
            block = hall.at[k, turn(y, o, NY)]
            remote(block, block, h_s.at[k, o], h_r.at[k, o], me).wait_recv()
        for j in range(NY):
            h, half = j // 2, j % 2
            ht[h * FEATS:(h + 1) * FEATS, half * 128:(half + 1) * 128] = hall[k, j].T

        def pick(i, _):
            low, high = split(oall[i, k:k + 1, :])
            tokens = lax.broadcasted_iota(jnp.int32, (LO, TERMS), 0)
            chosen = jnp.where(tokens == low, 1.0, 0.0).astype(BF16)
            four = jnp.dot(ht[...], chosen, preferred_element_type=F32)
            a, b, e, d = (four[h * FEATS:(h + 1) * FEATS] for h in range(HI))
            one = jnp.where(high < 2, jnp.where(high == 0, a, b), jnp.where(high == 2, e, d))
            rows[k, i] = one.astype(BF16)
            lpart[i, k:k + 1, 0:TERMS] = jnp.sum(one * wall[i].astype(F32), axis=0, keepdims=True)
            return 0

        lax.fori_loop(0, NX, pick, 0)

    for o in range(1, NX):
        x_copy(lpart.at[turn(x, o, NX)], lrecv.at[x], l_s, l_r, o).start()
    lrecv[x] = lpart[x]
    for o in range(1, NX):
        i = turn(x, o, NX)
        remote(lpart.at[i], lrecv.at[i], l_s.at[o], l_r.at[o], me).wait_recv()
    total = lrecv[0] + lrecv[1] + lrecv[2] + lrecv[3]
    lane = lax.broadcasted_iota(jnp.int32, (DOCS, WIDE), 1)
    zbuf[z] = jnp.where(lane < TERMS, total, count)
    for o in range(1, NZ):
        mine = zbuf.at[z]
        remote(mine, mine, z_s.at[o], z_r.at[NZ - o], dev(c, turn(z, o, NZ), y, x)).start()
    for o in range(1, NZ):
        theirs = zbuf.at[turn(z, o, NZ)]
        remote(theirs, theirs, z_s.at[o], z_r.at[o], me).wait_recv()
    total = zbuf[0]
    for i in range(1, NZ):
        total = total + zbuf[i]
    length = jnp.sum(jnp.where(lane == TERMS, total, 0.0), axis=1, keepdims=True)
    logits = total[:, 0:TERMS]
    validity = jnp.where(own[...].astype(F32) < length, 1.0, 0.0)
    soft = jnp.maximum(logits, 0.0) + jnp.log1p(jnp.exp(-jnp.abs(logits)))
    pooled = validity * jnp.log1p(soft)
    slopes = validity * jax.nn.sigmoid(logits) / (1.0 + soft)
    query, gap = pooled[0:1], pooled[1:2] - pooled[2:3]
    ubuf[x, 0:1, 0:TERMS] = (gap * slopes[0:1]).astype(BF16).astype(F32)
    ubuf[x, 1:2, 0:TERMS] = (query * slopes[1:2]).astype(BF16).astype(F32)
    ubuf[x, 2:3, 0:TERMS] = (-query * slopes[2:3]).astype(BF16).astype(F32)
    score = jnp.sum(query * gap, axis=1, keepdims=True)
    ubuf[x, 3:4, :] = jnp.broadcast_to(score, (1, WIDE))
    for o in range(1, NX):
        x_copy(ubuf.at[x], ubuf.at[x], u_s, u_r, o).start()
    for o in range(1, NX):
        i = turn(x, o, NX)
        remote(ubuf.at[i], ubuf.at[i], u_s.at[o], u_r.at[o], me).wait_recv()
    part = ubuf[0, 3:4, 0:128] + ubuf[1, 3:4, 0:128] + ubuf[2, 3:4, 0:128] + ubuf[3, 3:4, 0:128]
    ybuf[y] = jnp.broadcast_to(part, (8, 128))
    for o in range(1, NY):
        mine = ybuf.at[y]
        remote(mine, mine, y_s.at[o], y_r.at[NY - o], dev(c, z, turn(y, o, NY), x)).start()

    for k in range(DOCS):
        pacc[...] = jnp.zeros_like(pacc)

        def place(i, _):
            low, high = split(oall[i, k:k + 1, :])
            tokens = lax.broadcasted_iota(jnp.int32, (LO, TERMS), 0)
            spread = jnp.where(tokens == low, ubuf[i, k:k + 1, 0:TERMS], 0.0).astype(BF16)
            head = wall[i].astype(F32)
            cut = jnp.concatenate([jnp.where(high == h, head, 0.0).astype(BF16) for h in range(HI)], axis=0)
            pacc[...] += lax.dot_general(spread, cut, (((1,), (1,)), ((), ())), preferred_element_type=F32)
            return 0

        lax.fori_loop(0, NX, place, 0)
        for j in range(NY):
            h, half = j // 2, j % 2
            pk[k, j] = pacc[half * 128:(half + 1) * 128, h * FEATS:(h + 1) * FEATS].astype(BF16)
        for o in range(1, NY):
            j = turn(y, o, NY)
            remote(pk.at[k, j], precv.at[k, y], p_s.at[k, o], p_r.at[k, NY - o], dev(c, z, j, x)).start()

    for o in range(1, NY):
        theirs = ybuf.at[turn(y, o, NY)]
        remote(theirs, theirs, y_s.at[o], y_r.at[o], me).wait_recv()
    score = ybuf[0, 0:1, :]
    for i in range(1, NY):
        score = score + ybuf[i, 0:1, :]
    margin = ((score - teacher[0]) / scale)[:, 0:1]

    def head_part(i, _):
        a = ubuf[i, 0:1, 0:TERMS] * rows[0, i].astype(F32)
        b = ubuf[i, 1:2, 0:TERMS] * rows[1, i].astype(F32)
        d = ubuf[i, 2:3, 0:TERMS] * rows[2, i].astype(F32)
        ghb[i] = ((a + b + d) * margin).astype(BF16)
        return 0

    lax.fori_loop(0, NX, head_part, 0)
    half = FEATS // 2
    other = ghb.at[:, pl.ds(pl.multiple_of((1 - c) * half, half), half), :]
    swap = remote(other, ghr, c_s.at[0], c_r.at[0], dev(1 - c, z, y, x))
    swap.start()
    swap.wait_recv()

    def head_sum(i, _):
        mine = ghb[i, pl.ds(pl.multiple_of(c * half, half), half), :]
        ghx[i] = (mine.astype(F32) + ghr[i].astype(F32)).astype(BF16)
        return 0

    lax.fori_loop(0, NX, head_sum, 0)
    place_of = pl.ds(pl.multiple_of(x * FEATS + c * half, half), half)

    def head_copy(o, flip):
        cc = 1 - c if flip else c
        i = turn(x, o, NX)
        f = int(flip)
        return remote(
            ghx.at[i], gh_out.at[place_of, :], g_s.at[f, o], g_r.at[f, (NX - o) % NX], dev(cc, z, y, i)
        )

    head_moves = [(o, flip) for o in (2, 1, 3, 0) for flip in (False, True) if o or flip]
    for o, flip in head_moves:
        head_copy(o, flip).start()
    gh_out[place_of, :] = ghx[x]

    for k in range(DOCS):
        for o in range(1, NY):
            theirs = precv.at[k, turn(y, o, NY)]
            remote(theirs, theirs, p_s.at[k, o], p_r.at[k, o], me).wait_recv()
        precv[k, y] = pk[k, y]
        total = precv[k, 0].astype(F32)
        for j in range(1, NY):
            total = total + precv[k, j].astype(F32)
        fin[k] = (total * margin).astype(BF16)

    @pl.when(diagonal)
    def _():
        return_local().start()

    @pl.when(jnp.logical_not(diagonal))
    def _():
        return_copy(0).start()

    for o in range(1, NY):
        return_copy(o).start()

    for o, flip in head_moves:
        f = int(flip)
        remote(ghx.at[0], gh_out.at[pl.ds(0, half), :], g_s.at[f, o], g_r.at[f, o], me).wait_recv()
        head_copy(o, flip).wait_send()

    @pl.when(diagonal)
    def _():
        return_local().wait()

    @pl.when(jnp.logical_not(diagonal))
    def _():
        return_copy(0).wait_send()
        remote(fin.at[:, pl.ds(0, PIECE), :], gx_out.at[:, pl.ds(0, PIECE), :], f_s.at[0], f_r.at[0], me).wait_recv()

    for o in range(1, NY):
        remote(fin.at[:, pl.ds(0, PIECE), :], gx_out.at[:, pl.ds(0, PIECE), :], f_s.at[o], f_r.at[o], me).wait_recv()
        return_copy(o).wait_send()
        scatter_copy(o).wait_send()
    swap.wait_send()
    for o in range(1, NX):
        i = turn(x, o, NX)
        x_copy(own, oall.at[x], o_s, o_r, o).wait_send()
        x_copy(w.at[pl.ds(0, FEATS), :], wall.at[x], w_s, w_r, o).wait_send()
        x_copy(lpart.at[i], lrecv.at[x], l_s, l_r, o).wait_send()
        x_copy(ubuf.at[x], ubuf.at[x], u_s, u_r, o).wait_send()
    for o in range(1, NY):
        remote(zbuf.at[z], zbuf.at[z], z_s.at[o], z_r.at[o], me).wait_send()
        remote(ybuf.at[y], ybuf.at[y], y_s.at[o], y_r.at[o], me).wait_send()
        for k in range(DOCS):
            spread_copy(k, o).wait_send()
            remote(pk.at[k, 0], precv.at[k, y], p_s.at[k, o], p_r.at[k, o], me).wait_send()


def on_device(hidden_states, head_weight, owner_pos, token_ids, teacher_margin):
    scale = float(teacher_margin.shape[0] * NC)
    dma = pltpu.SemaphoreType.DMA
    vmem = pl.BlockSpec(memory_space=pltpu.VMEM)
    scratch = [
        pltpu.VMEM((NX, FEATS, TERMS), BF16),
        pltpu.VMEM((NX, DOCS, TERMS), jnp.int32),
        pltpu.VMEM((DOCS, NY, 128, FEATS), BF16),
        pltpu.VMEM((HI * FEATS, LO), BF16),
        pltpu.VMEM((DOCS, NX, FEATS, TERMS), BF16),
        pltpu.VMEM((NX, DOCS, WIDE), F32),
        pltpu.VMEM((NX, DOCS, WIDE), F32),
        pltpu.VMEM((NZ, DOCS, WIDE), F32),
        pltpu.VMEM((NX, DOCS + 1, WIDE), F32),
        pltpu.VMEM((NY, 8, 128), F32),
        pltpu.VMEM((LO, HI * FEATS), F32),
        pltpu.VMEM((DOCS, NY, 128, FEATS), BF16),
        pltpu.VMEM((DOCS, NY, 128, FEATS), BF16),
        pltpu.VMEM((NX, FEATS, TERMS), BF16),
        pltpu.VMEM((NX, FEATS // 2, TERMS), BF16),
        pltpu.VMEM((NX, FEATS // 2, TERMS), BF16),
        pltpu.VMEM((DOCS, 128, FEATS), BF16),
        dma((NX,)), dma((NX,)),
        dma((NX,)), dma((NX,)),
        dma((NY,)), dma((NY,)),
        dma((DOCS, NY)), dma((DOCS, NY)),
        dma((NX,)), dma((NX,)),
        dma((NZ,)), dma((NZ,)),
        dma((NX,)), dma((NX,)),
        dma((NY,)), dma((NY,)),
        dma((DOCS, NY)), dma((DOCS, NY)),
        dma((1,)), dma((1,)),
        dma((2, NX)), dma((2, NX)),
        dma((NY,)), dma((NY,)),
        dma((2,)),
    ]
    grad_head, grad_hidden = pl.pallas_call(
        functools.partial(kernel, scale),
        out_shape=(
            jax.ShapeDtypeStruct(head_weight.shape, BF16),
            jax.ShapeDtypeStruct(hidden_states.shape, BF16),
        ),
        in_specs=[vmem, vmem, vmem, vmem, pl.BlockSpec(memory_space=pltpu.SMEM)],
        out_specs=(vmem, vmem),
        scratch_shapes=scratch,
        compiler_params=pltpu.CompilerParams(collective_id=0, has_side_effects=True),
    )(hidden_states, head_weight, owner_pos, token_ids, teacher_margin)
    return grad_head.astype(F32), grad_hidden


def solution(mesh):
    return jax.shard_map(
        on_device,
        mesh=mesh,
        in_specs=(
            P("dp", "seq", "vocab"),
            P("seq", "vocab"),
            P("dp", "vocab"),
            P("dp", "seq"),
            P("dp"),
        ),
        out_specs=(P("seq", "vocab"), P("dp", "seq", "vocab")),
        check_vma=False,
    )
```

```python
import functools

import jax
import jax.numpy as jnp
from jax import lax
from jax.experimental import pallas as pl
from jax.experimental.pallas import tpu as pltpu
from jax.sharding import PartitionSpec as P

MESH = pl.DeviceIdType.MESH
F32 = jnp.float32
BF16 = jnp.bfloat16
NX, NY, NZ, NC = 4, 8, 8, 2
DOCS = 3
LO, HI = 256, 4
FEATS = 128
TERMS = 1000
WIDE = 1024
PIECE = 16


def kernel(
    scale, hid, w, own, tok, teacher, gh_out, gx_out,
    wt, wall, oall, hall, ht, rows, lpart, lrecv, zbuf, ubuf, ybuf, pacc, pk, relay_in, relay_out, precv, ghb, ghr, ghx, fin,
    w_s, w_r, o_s, o_r, s1_s, s1_r, h_s, h_r, l_s, l_r, z_s, z_r, u_s, u_r, y_s, y_r,
    p_s, p_r, c_s, c_r, g_s, g_r, k_s, k_r, f_s, f_r, loc,
):
    c = lax.axis_index("dp")
    z = lax.axis_index("seq")
    v = lax.axis_index("vocab")
    y, x = v // NX, lax.rem(v, NX)

    def dev(cc, zz, yy, xx):
        return (cc, zz, yy * NX + xx)

    def turn(i, o, n):
        return lax.rem(i + o + n, n)

    def remote(src, dst, ss, rs, to):
        return pltpu.make_async_remote_copy(
            src_ref=src, dst_ref=dst, send_sem=ss, recv_sem=rs, device_id=to, device_id_type=MESH
        )

    me = dev(c, z, y, x)
    diagonal = y == z
    lane_block = pl.ds(pl.multiple_of(x * FEATS, FEATS), FEATS)

    def piece(i):
        return pl.ds(pl.multiple_of(PIECE * i, PIECE), PIECE)

    def x_copy(src, dst, ss, rs, o):
        to = dev(c, z, y, turn(x, o, NX))
        return remote(src, dst, ss.at[o], rs.at[NX - o], to)

    def y_dev(o):
        return dev(c, z, turn(y, o, NY), x)

    def scatter(k, e, o):
        j = turn(y, o, NY)
        b = turn(j, 4 * e, NY)
        src, dst = hid.at[k, piece(b), :], hall.at[k, b, piece(z), :]

        def send():
            remote(src, dst, s1_s.at[k, e], s1_r.at[k, e], dev(c, y, j, x)).start()

        if o:
            send()
        else:
            pl.when(jnp.logical_not(diagonal))(send)

            @pl.when(diagonal)
            def _():
                pltpu.make_async_copy(src, dst, s1_r.at[k, e]).start()

    SPREAD = [(1, 0), (-1, 0), (1, 1), (-1, 1), (2, 0), (-2, 0)]

    def spread(k, n):
        o, e = SPREAD[n]
        block = hall.at[k, turn(y, 4 * e, NY)]
        return remote(block, block, h_s.at[k, n], h_r.at[k, n], y_dev(o))

    def send_home(k, o):
        zz = turn(z, o, NZ)
        src, dst = fin.at[k, piece(zz), :], gx_out.at[k, piece(y), :]

        def send():
            remote(src, dst, f_s.at[k], f_r.at[k], dev(c, zz, z, x)).start()

        if o:
            send()
        else:
            pl.when(jnp.logical_not(diagonal))(send)

            @pl.when(diagonal)
            def _():
                pltpu.make_async_copy(src, dst, f_r.at[k]).start()

    barrier = pltpu.get_barrier_semaphore()

    def greet(to):
        pl.semaphore_signal(barrier, inc=1, device_id=to, device_id_type=MESH)

    for o in range(NY):
        greet(dev(c, y, turn(y, o, NY), x))
        greet(dev(c, turn(z, o, NZ), z, x))
    for o in range(1, NY):
        greet(dev(c, z, turn(y, o, NY), x))
        greet(dev(c, turn(z, o, NZ), y, x))
    for o in range(1, NX):
        greet(dev(c, z, y, turn(x, o, NX)))
    greet(dev(1 - c, z, y, x))

    own_head = pltpu.make_async_copy(w.at[:, lane_block], wt.at[x], loc.at[0])
    own_head.start()
    oall[x] = own[...]
    lpart[...] = jnp.zeros_like(lpart)
    ghb[...] = jnp.zeros_like(ghb)
    count = jnp.sum((tok[...] != 0).astype(F32), axis=1, keepdims=True)
    pl.semaphore_wait(barrier, 2 * NY + 2 * (NY - 1) + (NX - 1) + 1)

    for k in range(DOCS):
        for o in range(NY):
            for e in range(2):
                scatter(k, e, o)
    for o in range(1, NX):
        x_copy(own, oall.at[x], o_s, o_r, o).start()
    for o in range(1, NX):
        i = turn(x, o, NX)
        src = w.at[:, pl.ds(pl.multiple_of(i * FEATS, FEATS), FEATS)]
        x_copy(src, wt.at[x], w_s, w_r, o).start()

    for k in range(DOCS):
        for e in range(2):
            block = hall.at[k, turn(y, 4 * e, NY)]
            pltpu.make_async_copy(block, block, s1_r.at[k, e]).wait()
        for n in range(len(SPREAD)):
            spread(k, n).start()

    own_head.wait()
    wall[x] = wt[x].T
    for o in (1, 3, 2):
        i = turn(x, o, NX)
        remote(own, oall.at[i], o_s.at[o], o_r.at[o], me).wait_recv()
        remote(wt.at[i], wt.at[i], w_s.at[o], w_r.at[o], me).wait_recv()
        wall[i] = wt[i].T

    def split(owner):
        low = ((owner >> 4) & 1) * 128 + (owner >> 7) * PIECE + (owner & (PIECE - 1))
        return low, (owner >> 5) & 3

    for k in range(DOCS):
        for n in range(len(SPREAD)):
            o, e = SPREAD[n]
            block = hall.at[k, turn(y, 4 * e - o, NY)]
            remote(block, block, h_s.at[k, n], h_r.at[k, n], me).wait_recv()
        for j in range(NY):
            h, half = j // 2, j % 2
            ht[h * FEATS:(h + 1) * FEATS, half * 128:(half + 1) * 128] = hall[k, j].T

        def pick(i, _):
            low, high = split(oall[i, k:k + 1, :])
            tokens = lax.broadcasted_iota(jnp.int32, (LO, TERMS), 0)
            chosen = jnp.where(tokens == low, 1.0, 0.0).astype(BF16)
            four = jnp.dot(ht[...], chosen, preferred_element_type=F32)
            a, b, e, d = (four[h * FEATS:(h + 1) * FEATS] for h in range(HI))
            one = jnp.where(high < 2, jnp.where(high == 0, a, b), jnp.where(high == 2, e, d))
            rows[k, i] = one.astype(BF16)
            lpart[i, k:k + 1, 0:TERMS] = jnp.sum(one * wall[i].astype(F32), axis=0, keepdims=True)
            return 0

        lax.fori_loop(0, NX, pick, 0)

    for o in range(1, NX):
        x_copy(lpart.at[turn(x, o, NX)], lrecv.at[x], l_s, l_r, o).start()
    lrecv[x] = lpart[x]
    for o in range(1, NX):
        i = turn(x, o, NX)
        remote(lpart.at[i], lrecv.at[i], l_s.at[o], l_r.at[o], me).wait_recv()
    total = lrecv[0] + lrecv[1] + lrecv[2] + lrecv[3]
    lane = lax.broadcasted_iota(jnp.int32, (DOCS, WIDE), 1)
    zbuf[z] = jnp.where(lane < TERMS, total, count)
    for o in range(1, NZ):
        mine = zbuf.at[z]
        remote(mine, mine, z_s.at[o], z_r.at[NZ - o], dev(c, turn(z, o, NZ), y, x)).start()
    for o in range(1, NZ):
        theirs = zbuf.at[turn(z, o, NZ)]
        remote(theirs, theirs, z_s.at[o], z_r.at[o], me).wait_recv()
    total = zbuf[0]
    for i in range(1, NZ):
        total = total + zbuf[i]
    length = jnp.sum(jnp.where(lane == TERMS, total, 0.0), axis=1, keepdims=True)
    logits = total[:, 0:TERMS]
    validity = jnp.where(own[...].astype(F32) < length, 1.0, 0.0)
    soft = jnp.maximum(logits, 0.0) + jnp.log1p(jnp.exp(-jnp.abs(logits)))
    pooled = validity * jnp.log1p(soft)
    slopes = validity * jax.nn.sigmoid(logits) / (1.0 + soft)
    query, gap = pooled[0:1], pooled[1:2] - pooled[2:3]
    ubuf[x, 0:1, 0:TERMS] = (gap * slopes[0:1]).astype(BF16).astype(F32)
    ubuf[x, 1:2, 0:TERMS] = (query * slopes[1:2]).astype(BF16).astype(F32)
    ubuf[x, 2:3, 0:TERMS] = (-query * slopes[2:3]).astype(BF16).astype(F32)
    score = jnp.sum(query * gap, axis=1, keepdims=True)
    ubuf[x, 3:4, :] = jnp.broadcast_to(score, (1, WIDE))
    for o in range(1, NX):
        x_copy(ubuf.at[x], ubuf.at[x], u_s, u_r, o).start()
    for o in range(1, NX):
        i = turn(x, o, NX)
        remote(ubuf.at[i], ubuf.at[i], u_s.at[o], u_r.at[o], me).wait_recv()
    part = ubuf[0, 3:4, 0:128] + ubuf[1, 3:4, 0:128] + ubuf[2, 3:4, 0:128] + ubuf[3, 3:4, 0:128]
    ybuf[y] = jnp.broadcast_to(part, (8, 128))
    for o in range(1, NY):
        mine = ybuf.at[y]
        remote(mine, mine, y_s.at[o], y_r.at[NY - o], y_dev(o)).start()

    def far_side(k):
        return 1 if k % 2 == 0 else -1

    def first_sends(k):
        f = far_side(k)
        return [
            remote(pk.at[k, turn(y, -3, NY)], relay_in.at[k, 0], p_s.at[k, 0], p_r.at[k, 0], y_dev(-1)),
            remote(pk.at[k, turn(y, 3, NY)], relay_in.at[k, 1], p_s.at[k, 1], p_r.at[k, 1], y_dev(1)),
            remote(pk.at[k, turn(y, 4, NY)], relay_in.at[k, 2], p_s.at[k, 2], p_r.at[k, 2], y_dev(-2 * f)),
            remote(pk.at[k, turn(y, -1, NY)], precv.at[k, 0], p_s.at[k, 3], p_r.at[k, 3], y_dev(-1)),
            remote(pk.at[k, turn(y, 1, NY)], precv.at[k, 1], p_s.at[k, 4], p_r.at[k, 4], y_dev(1)),
        ]

    def relay_sends(k):
        return [
            remote(relay_out.at[k, 0], precv.at[k, 2], p_s.at[k, 5], p_r.at[k, 5], y_dev(-2)),
            remote(relay_out.at[k, 1], precv.at[k, 3], p_s.at[k, 6], p_r.at[k, 6], y_dev(2)),
        ]

    def block_terms(k):
        pacc[...] = jnp.zeros_like(pacc)

        def place(i, _):
            low, high = split(oall[i, k:k + 1, :])
            tokens = lax.broadcasted_iota(jnp.int32, (LO, TERMS), 0)
            spread_out = jnp.where(tokens == low, ubuf[i, k:k + 1, 0:TERMS], 0.0).astype(BF16)
            head = wall[i].astype(F32)
            cut = jnp.concatenate([jnp.where(high == h, head, 0.0).astype(BF16) for h in range(HI)], axis=0)
            pacc[...] += lax.dot_general(spread_out, cut, (((1,), (1,)), ((), ())), preferred_element_type=F32)
            return 0

        lax.fori_loop(0, NX, place, 0)
        for j in range(NY):
            h, half = j // 2, j % 2
            pk[k, j] = pacc[half * 128:(half + 1) * 128, h * FEATS:(h + 1) * FEATS].astype(BF16)
        for move in first_sends(k):
            move.start()

    def relay(k):
        for n in range(3):
            remote(relay_in.at[k, n], relay_in.at[k, n], p_s.at[k, n], p_r.at[k, n], me).wait_recv()
        far = relay_in[k, 2].astype(F32)
        for n, o in ((0, -2), (1, 2)):
            total = pk[k, turn(y, o, NY)].astype(F32) + relay_in[k, n].astype(F32)
            if (far_side(k) == 1) == (n == 0):
                total = total + far
            relay_out[k, n] = total.astype(BF16)
        for move in relay_sends(k):
            move.start()

    def gather_home(k):
        for n in range(4):
            remote(precv.at[k, n], precv.at[k, n], p_s.at[k, 3 + n], p_r.at[k, 3 + n], me).wait_recv()
        total = pk[k, y].astype(F32)
        for n in range(4):
            total = total + precv[k, n].astype(F32)
        fin[k] = (total * margin).astype(BF16)
        for o in range(NZ):
            send_home(k, o)

    block_terms(0)
    block_terms(1)
    relay(0)
    block_terms(2)

    for o in range(1, NY):
        theirs = ybuf.at[turn(y, o, NY)]
        remote(theirs, theirs, y_s.at[o], y_r.at[o], me).wait_recv()
    score = ybuf[0, 0:1, :]
    for i in range(1, NY):
        score = score + ybuf[i, 0:1, :]
    margin = ((score - teacher[0]) / scale)[:, 0:1]

    def head_part(i, _):
        a = ubuf[i, 0:1, 0:TERMS] * rows[0, i].astype(F32)
        b = ubuf[i, 1:2, 0:TERMS] * rows[1, i].astype(F32)
        d = ubuf[i, 2:3, 0:TERMS] * rows[2, i].astype(F32)
        ghb[i, 0:TERMS, :] = ((a + b + d) * margin).astype(BF16).T
        return 0

    lax.fori_loop(0, NX, head_part, 0)
    half = WIDE // 2
    mine_half = pl.ds(pl.multiple_of(c * half, half), half)
    other_half = pl.ds(pl.multiple_of((1 - c) * half, half), half)
    swap = remote(ghb.at[:, other_half, :], ghr, c_s.at[0], c_r.at[0], dev(1 - c, z, y, x))
    swap.start()
    relay(1)
    gather_home(0)
    swap.wait_recv()

    def head_sum(i, _):
        ghx[i] = (ghb[i, mine_half, :].astype(F32) + ghr[i].astype(F32)).astype(BF16)
        return 0

    lax.fori_loop(0, NX, head_sum, 0)

    def head_copy(o):
        return x_copy(ghx.at[turn(x, o, NX)], gh_out.at[mine_half, lane_block], g_s, g_r, o)

    for o in (2, 1, 3):
        head_copy(o).start()
    own_out = remote(ghx.at[x], gh_out.at[mine_half, lane_block], k_s.at[0], k_r.at[0], dev(1 - c, z, y, x))
    own_out.start()
    gh_out[mine_half, lane_block] = ghx[x]

    def forward(o):
        i = turn(x, o, NX)
        block = gh_out.at[mine_half, pl.ds(pl.multiple_of(i * FEATS, FEATS), FEATS)]
        return remote(block, block, k_s.at[o], k_r.at[o], dev(1 - c, z, y, x))

    relay(2)
    gather_home(1)
    gather_home(2)

    for o in (1, 3, 2):
        head_copy(o).wait_send()
        i = turn(x, o, NX)
        block = gh_out.at[mine_half, pl.ds(pl.multiple_of(i * FEATS, FEATS), FEATS)]
        remote(ghx.at[0], block, g_s.at[o], g_r.at[o], me).wait_recv()
        forward(o).start()

    for k in range(DOCS):
        pltpu.make_async_copy(fin.at[k], gx_out.at[k], f_r.at[k]).wait()
    for o in range(NX):
        i = turn(x, o, NX)
        block = gh_out.at[other_half, pl.ds(pl.multiple_of(i * FEATS, FEATS), FEATS)]
        remote(ghx.at[0], block, k_s.at[o], k_r.at[o], me).wait()
    swap.wait_send()
    for o in range(1, NX):
        i = turn(x, o, NX)
        x_copy(own, oall.at[x], o_s, o_r, o).wait_send()
        x_copy(wt.at[i], wt.at[i], w_s, w_r, o).wait_send()
        x_copy(lpart.at[i], lrecv.at[x], l_s, l_r, o).wait_send()
        x_copy(ubuf.at[x], ubuf.at[x], u_s, u_r, o).wait_send()
    for o in range(1, NY):
        remote(zbuf.at[z], zbuf.at[z], z_s.at[o], z_r.at[o], me).wait_send()
        remote(ybuf.at[y], ybuf.at[y], y_s.at[o], y_r.at[o], me).wait_send()
    for k in range(DOCS):
        for n in range(len(SPREAD)):
            spread(k, n).wait_send()
        for move in first_sends(k) + relay_sends(k):
            move.wait_send()

        def drain(n):
            size = pl.ds(0, n * PIECE)
            remote(fin.at[k, size, :], fin.at[k, size, :], f_s.at[k], f_r.at[k], me).wait_send()
            for e in range(2):
                remote(hid.at[k, size, :], hid.at[k, size, :], s1_s.at[k, e], s1_r.at[k, e], me).wait_send()

        pl.when(diagonal)(functools.partial(drain, NY - 1))
        pl.when(jnp.logical_not(diagonal))(functools.partial(drain, NY))


def on_device(hidden_states, head_weight, owner_pos, token_ids, teacher_margin):
    scale = float(teacher_margin.shape[0] * NC)
    dma = pltpu.SemaphoreType.DMA
    vmem = pl.BlockSpec(memory_space=pltpu.VMEM)
    scratch = [
        pltpu.VMEM((NX, TERMS, FEATS), BF16),
        pltpu.VMEM((NX, FEATS, TERMS), BF16),
        pltpu.VMEM((NX, DOCS, TERMS), jnp.int32),
        pltpu.VMEM((DOCS, NY, 128, FEATS), BF16),
        pltpu.VMEM((HI * FEATS, LO), BF16),
        pltpu.VMEM((DOCS, NX, FEATS, TERMS), BF16),
        pltpu.VMEM((NX, DOCS, WIDE), F32),
        pltpu.VMEM((NX, DOCS, WIDE), F32),
        pltpu.VMEM((NZ, DOCS, WIDE), F32),
        pltpu.VMEM((NX, DOCS + 1, WIDE), F32),
        pltpu.VMEM((NY, 8, 128), F32),
        pltpu.VMEM((LO, HI * FEATS), F32),
        pltpu.VMEM((DOCS, NY, 128, FEATS), BF16),
        pltpu.VMEM((DOCS, 3, 128, FEATS), BF16),
        pltpu.VMEM((DOCS, 2, 128, FEATS), BF16),
        pltpu.VMEM((DOCS, 4, 128, FEATS), BF16),
        pltpu.VMEM((NX, WIDE, FEATS), BF16),
        pltpu.VMEM((NX, WIDE // 2, FEATS), BF16),
        pltpu.VMEM((NX, WIDE // 2, FEATS), BF16),
        pltpu.VMEM((DOCS, 128, FEATS), BF16),
        dma((NX,)), dma((NX,)),
        dma((NX,)), dma((NX,)),
        dma((DOCS, 2)), dma((DOCS, 2)),
        dma((DOCS, 6)), dma((DOCS, 6)),
        dma((NX,)), dma((NX,)),
        dma((NZ,)), dma((NZ,)),
        dma((NX,)), dma((NX,)),
        dma((NY,)), dma((NY,)),
        dma((DOCS, 7)), dma((DOCS, 7)),
        dma((1,)), dma((1,)),
        dma((NX,)), dma((NX,)),
        dma((NX,)), dma((NX,)),
        dma((DOCS,)), dma((DOCS,)),
        dma((1,)),
    ]
    grad_head, grad_hidden = pl.pallas_call(
        functools.partial(kernel, scale),
        out_shape=(
            jax.ShapeDtypeStruct((WIDE, head_weight.shape[0]), BF16),
            jax.ShapeDtypeStruct(hidden_states.shape, BF16),
        ),
        in_specs=[vmem, pl.BlockSpec(memory_space=pl.ANY), vmem, vmem, pl.BlockSpec(memory_space=pltpu.SMEM)],
        out_specs=(vmem, vmem),
        scratch_shapes=scratch,
        compiler_params=pltpu.CompilerParams(collective_id=0, has_side_effects=True),
    )(hidden_states, head_weight.T, owner_pos, token_ids, teacher_margin)
    return grad_head[:TERMS].astype(F32).T, grad_hidden


def solution(mesh):
    return jax.shard_map(
        on_device,
        mesh=mesh,
        in_specs=(
            P("dp", "seq", "vocab"),
            P("seq", "vocab"),
            P("dp", "vocab"),
            P("dp", "seq"),
            P("dp"),
        ),
        out_specs=(P("seq", "vocab"), P("dp", "seq", "vocab")),
        check_vma=False,
    )
```

```python
import functools

import jax
import jax.numpy as jnp
from jax import lax
from jax.experimental import pallas as pl
from jax.experimental.pallas import tpu as pltpu
from jax.sharding import PartitionSpec as P

MESH = pl.DeviceIdType.MESH
F32 = jnp.float32
BF16 = jnp.bfloat16
NX, NY, NZ, NC = 4, 8, 8, 2
DOCS = 3
LO, HI = 256, 4
FEATS = 128
TERMS = 1000
WIDE = 1024
PIECE = 16
TAKEN = 504
VMEM_LIMIT = 32 * 1024 * 1024


def kernel(
    scale, hid, w, own_in, tok_in, teacher, gh_out, gx_out,
    own, tok, wt, wall, oall, hall, ht, rows, lpart, lrecv, zbuf, ubuf, ybuf, pacc, pk, relay_in, relay_out, precv, ghb, ghr, ghx, mbuf, fin,
    w_s, w_r, o_s, o_r, s1_s, s1_r, h_s, h_r, l_s, l_r, z_s, z_r, u_s, u_r, y_s, y_r,
    p_s, p_r, c_s, c_r, g_s, g_r, k_s, k_r, f_s, f_r, q_s, q_r, loc,
):
    c = lax.axis_index("dp")
    z = lax.axis_index("seq")
    v = lax.axis_index("vocab")
    y, x = v // NX, lax.rem(v, NX)

    def dev(cc, zz, yy, xx):
        return (cc, zz, yy * NX + xx)

    def turn(i, o, n):
        return lax.rem(i + o + n, n)

    def remote(src, dst, ss, rs, to):
        return pltpu.make_async_remote_copy(
            src_ref=src, dst_ref=dst, send_sem=ss, recv_sem=rs, device_id=to, device_id_type=MESH
        )

    me = dev(c, z, y, x)
    diagonal = y == z
    lane_block = pl.ds(pl.multiple_of(x * FEATS, FEATS), FEATS)

    def piece(i):
        return pl.ds(pl.multiple_of(PIECE * i, PIECE), PIECE)

    def x_copy(src, dst, ss, rs, o):
        to = dev(c, z, y, turn(x, o, NX))
        return remote(src, dst, ss.at[o], rs.at[NX - o], to)

    def y_dev(o):
        return dev(c, z, turn(y, o, NY), x)

    def scatter(k, e, o):
        j = turn(y, o, NY)
        b = turn(j, 4 * e, NY)
        src, dst = hid.at[k, piece(b), :], hall.at[k, b, piece(z), :]

        def send():
            remote(src, dst, s1_s.at[k, e], s1_r.at[k, e], dev(c, y, j, x)).start()

        if o:
            send()
        else:
            pl.when(jnp.logical_not(diagonal))(send)

            @pl.when(diagonal)
            def _():
                pltpu.make_async_copy(src, dst, s1_r.at[k, e]).start()

    SPREAD = [(1, 0), (-1, 0), (1, 1), (-1, 1), (2, 0), (-2, 0)]

    def spread(k, n):
        o, e = SPREAD[n]
        block = hall.at[k, turn(y, 4 * e, NY)]
        return remote(block, block, h_s.at[k, n], h_r.at[k, n], y_dev(o))

    def send_home(k, o):
        zz = turn(z, o, NZ)
        src, dst = fin.at[k, piece(zz), :], gx_out.at[k, piece(y), :]

        def send():
            remote(src, dst, f_s.at[k], f_r.at[k], dev(c, zz, z, x)).start()

        if o:
            send()
        else:
            pl.when(jnp.logical_not(diagonal))(send)

            @pl.when(diagonal)
            def _():
                pltpu.make_async_copy(src, dst, f_r.at[k]).start()

    taken = pl.ds(pl.multiple_of(c * (TERMS - TAKEN), 8), TAKEN)
    given = pl.ds(pl.multiple_of(c * TAKEN, 8), TERMS - TAKEN)
    lacked = pl.ds(pl.multiple_of((1 - c) * TAKEN, 8), TERMS - TAKEN)

    def share(o):
        block = wt.at[turn(x, o, NX), given, :]
        return remote(block, block, q_s.at[o], q_r.at[o], dev(1 - c, z, y, x))

    barrier = pltpu.get_barrier_semaphore()

    def greet(to):
        pl.semaphore_signal(barrier, inc=1, device_id=to, device_id_type=MESH)

    own_load = pltpu.make_async_copy(own_in, own, loc.at[2])
    own_load.start()
    tok_load = pltpu.make_async_copy(tok_in, tok, loc.at[3])
    tok_load.start()
    own_head = pltpu.make_async_copy(w.at[:, lane_block], wt.at[x], loc.at[0])
    own_head.start()
    for o in range(NY):
        greet(dev(c, y, turn(y, o, NY), x))
        greet(dev(c, turn(z, o, NZ), z, x))
    for o in range(1, NY):
        greet(dev(c, z, turn(y, o, NY), x))
        greet(dev(c, turn(z, o, NZ), y, x))
    for o in range(1, NX):
        greet(dev(c, z, y, turn(x, o, NX)))
    greet(dev(1 - c, z, y, x))

    lpart[...] = jnp.zeros_like(lpart)
    ghb[...] = jnp.zeros_like(ghb)
    own_load.wait()
    tok_load.wait()
    oall[x] = own[...]
    count = jnp.sum((tok[...] != 0).astype(F32), axis=1, keepdims=True)
    pl.semaphore_wait(barrier, 2 * NY + 2 * (NY - 1) + (NX - 1) + 1)

    for k in range(DOCS):
        for o in range(NY):
            for e in range(2):
                scatter(k, e, o)
    for o in range(1, NX):
        x_copy(own, oall.at[x], o_s, o_r, o).start()
    for o in range(1, NX):
        i = turn(x, o, NX)
        src = w.at[taken, pl.ds(pl.multiple_of(i * FEATS, FEATS), FEATS)]
        x_copy(src, wt.at[x, taken, :], w_s, w_r, o).start()

    for k in range(DOCS):
        for e in range(2):
            block = hall.at[k, turn(y, 4 * e, NY)]
            pltpu.make_async_copy(block, block, s1_r.at[k, e]).wait()
        for n in range(len(SPREAD)):
            spread(k, n).start()

    def split(owner):
        low = ((owner >> 4) & 1) * 128 + (owner >> 7) * PIECE + (owner & (PIECE - 1))
        return low, (owner >> 5) & 3

    for o in (1, 3, 2):
        i = turn(x, o, NX)
        remote(own, oall.at[i], o_s.at[o], o_r.at[o], me).wait_recv()

    for k in range(DOCS):
        for n in range(len(SPREAD)):
            o, e = SPREAD[n]
            block = hall.at[k, turn(y, 4 * e - o, NY)]
            remote(block, block, h_s.at[k, n], h_r.at[k, n], me).wait_recv()
        for j in range(NY):
            h, half = j // 2, j % 2
            ht[h * FEATS:(h + 1) * FEATS, half * 128:(half + 1) * 128] = hall[k, j].T

        def pick(i, _):
            low, high = split(oall[i, k:k + 1, :])
            tokens = lax.broadcasted_iota(jnp.int32, (LO, TERMS), 0)
            chosen = jnp.where(tokens == low, 1.0, 0.0).astype(BF16)
            four = jnp.dot(ht[...], chosen, preferred_element_type=F32)
            a, b, e, d = (four[h * FEATS:(h + 1) * FEATS] for h in range(HI))
            one = jnp.where(high < 2, jnp.where(high == 0, a, b), jnp.where(high == 2, e, d))
            rows[k, i] = one.astype(BF16)
            return 0

        lax.fori_loop(0, NX, pick, 0)

        if k == 0:
            for o in (1, 3, 2):
                i = turn(x, o, NX)
                remote(wt.at[i, taken, :], wt.at[i, taken, :], w_s.at[o], w_r.at[o], me).wait_recv()
                share(o).start()

    own_head.wait()
    for o in (1, 3, 2):
        i = turn(x, o, NX)
        remote(wt.at[i, lacked, :], wt.at[i, lacked, :], q_s.at[o], q_r.at[o], me).wait_recv()

    def dots(i, _):
        block = wt[i].T
        wall[i] = block
        head = block.astype(F32)
        for k in range(DOCS):
            lpart[i, k:k + 1, 0:TERMS] = jnp.sum(rows[k, i].astype(F32) * head, axis=0, keepdims=True)
        return 0

    lax.fori_loop(0, NX, dots, 0)

    for o in range(1, NX):
        x_copy(lpart.at[turn(x, o, NX)], lrecv.at[x], l_s, l_r, o).start()
    lrecv[x] = lpart[x]
    for o in range(1, NX):
        i = turn(x, o, NX)
        remote(lpart.at[i], lrecv.at[i], l_s.at[o], l_r.at[o], me).wait_recv()
    total = lrecv[0] + lrecv[1] + lrecv[2] + lrecv[3]
    lane = lax.broadcasted_iota(jnp.int32, (DOCS, WIDE), 1)
    zbuf[z] = jnp.where(lane < TERMS, total, count)
    for o in range(1, NZ):
        mine = zbuf.at[z]
        remote(mine, mine, z_s.at[o], z_r.at[NZ - o], dev(c, turn(z, o, NZ), y, x)).start()
    for o in range(1, NZ):
        theirs = zbuf.at[turn(z, o, NZ)]
        remote(theirs, theirs, z_s.at[o], z_r.at[o], me).wait_recv()
    total = zbuf[0]
    for i in range(1, NZ):
        total = total + zbuf[i]
    length = jnp.sum(jnp.where(lane == TERMS, total, 0.0), axis=1, keepdims=True)
    logits = total[:, 0:TERMS]
    validity = jnp.where(own[...].astype(F32) < length, 1.0, 0.0)
    soft = jnp.maximum(logits, 0.0) + jnp.log1p(jnp.exp(-jnp.abs(logits)))
    pooled = validity * jnp.log1p(soft)
    slopes = validity * jax.nn.sigmoid(logits) / (1.0 + soft)
    query, gap = pooled[0:1], pooled[1:2] - pooled[2:3]
    ubuf[x, 0:1, 0:TERMS] = (gap * slopes[0:1]).astype(BF16).astype(F32)
    ubuf[x, 1:2, 0:TERMS] = (query * slopes[1:2]).astype(BF16).astype(F32)
    ubuf[x, 2:3, 0:TERMS] = (-query * slopes[2:3]).astype(BF16).astype(F32)
    score = jnp.sum(query * gap, axis=1, keepdims=True)
    ubuf[x, 3:4, :] = jnp.broadcast_to(score, (1, WIDE))
    for o in range(1, NX):
        x_copy(ubuf.at[x], ubuf.at[x], u_s, u_r, o).start()
    for o in range(1, NX):
        i = turn(x, o, NX)
        remote(ubuf.at[i], ubuf.at[i], u_s.at[o], u_r.at[o], me).wait_recv()
    part = ubuf[0, 3:4, 0:128] + ubuf[1, 3:4, 0:128] + ubuf[2, 3:4, 0:128] + ubuf[3, 3:4, 0:128]
    ybuf[y] = jnp.broadcast_to(part, (8, 128))
    for o in range(1, NY):
        mine = ybuf.at[y]
        remote(mine, mine, y_s.at[o], y_r.at[NY - o], y_dev(o)).start()

    def far_side(k):
        return 1 if k % 2 == 0 else -1

    def first_sends(k):
        f = far_side(k)
        return [
            remote(pk.at[k, turn(y, -3, NY)], relay_in.at[k, 0], p_s.at[k, 0], p_r.at[k, 0], y_dev(-1)),
            remote(pk.at[k, turn(y, 3, NY)], relay_in.at[k, 1], p_s.at[k, 1], p_r.at[k, 1], y_dev(1)),
            remote(pk.at[k, turn(y, 4, NY)], relay_in.at[k, 2], p_s.at[k, 2], p_r.at[k, 2], y_dev(-2 * f)),
            remote(pk.at[k, turn(y, -1, NY)], precv.at[k, 0], p_s.at[k, 3], p_r.at[k, 3], y_dev(-1)),
            remote(pk.at[k, turn(y, 1, NY)], precv.at[k, 1], p_s.at[k, 4], p_r.at[k, 4], y_dev(1)),
        ]

    def relay_sends(k):
        return [
            remote(relay_out.at[k, 0], precv.at[k, 2], p_s.at[k, 5], p_r.at[k, 5], y_dev(-2)),
            remote(relay_out.at[k, 1], precv.at[k, 3], p_s.at[k, 6], p_r.at[k, 6], y_dev(2)),
        ]

    def block_terms(k):
        pacc[...] = jnp.zeros_like(pacc)

        def place(i, _):
            low, high = split(oall[i, k:k + 1, :])
            tokens = lax.broadcasted_iota(jnp.int32, (LO, TERMS), 0)
            spread_out = jnp.where(tokens == low, ubuf[i, k:k + 1, 0:TERMS], 0.0).astype(BF16)
            head = wall[i].astype(F32)
            cut = jnp.concatenate([jnp.where(high == h, head, 0.0).astype(BF16) for h in range(HI)], axis=0)
            pacc[...] += lax.dot_general(spread_out, cut, (((1,), (1,)), ((), ())), preferred_element_type=F32)
            return 0

        lax.fori_loop(0, NX, place, 0)
        for j in range(NY):
            h, half = j // 2, j % 2
            pk[k, j] = pacc[half * 128:(half + 1) * 128, h * FEATS:(h + 1) * FEATS].astype(BF16)
        for move in first_sends(k):
            move.start()

    def relay(k):
        for n in range(3):
            remote(relay_in.at[k, n], relay_in.at[k, n], p_s.at[k, n], p_r.at[k, n], me).wait_recv()
        far = relay_in[k, 2].astype(F32)
        for n, o in ((0, -2), (1, 2)):
            total = pk[k, turn(y, o, NY)].astype(F32) + relay_in[k, n].astype(F32)
            if (far_side(k) == 1) == (n == 0):
                total = total + far
            relay_out[k, n] = total.astype(BF16)
        for move in relay_sends(k):
            move.start()

    def gather_home(k):
        for n in range(4):
            remote(precv.at[k, n], precv.at[k, n], p_s.at[k, 3 + n], p_r.at[k, 3 + n], me).wait_recv()
        total = pk[k, y].astype(F32)
        for n in range(4):
            total = total + precv[k, n].astype(F32)
        fin[k] = (total * margin).astype(BF16)
        for o in range(NZ):
            send_home(k, o)

    block_terms(0)

    def head_part(i, _):
        a = ubuf[i, 0:1, 0:TERMS] * rows[0, i].astype(F32)
        b = ubuf[i, 1:2, 0:TERMS] * rows[1, i].astype(F32)
        d = ubuf[i, 2:3, 0:TERMS] * rows[2, i].astype(F32)
        ghb[i, 0:TERMS, :] = (a + b + d).astype(BF16).T
        return 0

    lax.fori_loop(0, NX, head_part, 0)
    half = WIDE // 2
    mine_half = pl.ds(pl.multiple_of(c * half, half), half)
    other_half = pl.ds(pl.multiple_of((1 - c) * half, half), half)
    swap = remote(ghb.at[:, other_half, :], ghr, c_s.at[0], c_r.at[0], dev(1 - c, z, y, x))
    swap.start()

    block_terms(1)
    relay(0)
    block_terms(2)

    for o in range(1, NY):
        theirs = ybuf.at[turn(y, o, NY)]
        remote(theirs, theirs, y_s.at[o], y_r.at[o], me).wait_recv()
    score = ybuf[0, 0:1, :]
    for i in range(1, NY):
        score = score + ybuf[i, 0:1, :]
    scaled = (score - teacher[0]) / scale
    margin = scaled[:, 0:1]
    mbuf[0] = jnp.broadcast_to(scaled, (8, 128))
    tell = remote(mbuf.at[0], mbuf.at[1], c_s.at[1], c_r.at[1], dev(1 - c, z, y, x))
    tell.start()
    relay(1)
    gather_home(0)
    relay(2)
    gather_home(1)
    swap.wait_recv()
    tell.wait_recv()

    other_margin = mbuf[1, 0:1, 0:1]

    def head_sum(i, _):
        total = ghb[i, mine_half, :].astype(F32) * margin + ghr[i].astype(F32) * other_margin
        ghx[i] = total.astype(BF16)
        return 0

    lax.fori_loop(0, NX, head_sum, 0)

    def head_copy(o):
        return x_copy(ghx.at[turn(x, o, NX)], gh_out.at[mine_half, lane_block], g_s, g_r, o)

    for o in (2, 1, 3):
        head_copy(o).start()
    own_out = remote(ghx.at[x], gh_out.at[mine_half, lane_block], k_s.at[0], k_r.at[0], dev(1 - c, z, y, x))
    own_out.start()
    own_move = pltpu.make_async_copy(ghx.at[x], gh_out.at[mine_half, lane_block], loc.at[1])
    own_move.start()

    def forward(o):
        i = turn(x, o, NX)
        block = gh_out.at[mine_half, pl.ds(pl.multiple_of(i * FEATS, FEATS), FEATS)]
        return remote(block, block, k_s.at[o], k_r.at[o], dev(1 - c, z, y, x))

    gather_home(2)

    for o in (1, 3, 2):
        head_copy(o).wait_send()
        i = turn(x, o, NX)
        block = gh_out.at[mine_half, pl.ds(pl.multiple_of(i * FEATS, FEATS), FEATS)]
        remote(ghx.at[0], block, g_s.at[o], g_r.at[o], me).wait_recv()
        forward(o).start()

    for k in range(DOCS):
        pltpu.make_async_copy(fin.at[k], gx_out.at[k], f_r.at[k]).wait()
    for o in range(NX):
        i = turn(x, o, NX)
        block = gh_out.at[other_half, pl.ds(pl.multiple_of(i * FEATS, FEATS), FEATS)]
        remote(ghx.at[0], block, k_s.at[o], k_r.at[o], me).wait()
    swap.wait_send()
    tell.wait_send()
    own_move.wait()
    for o in range(1, NX):
        i = turn(x, o, NX)
        x_copy(own, oall.at[x], o_s, o_r, o).wait_send()
        x_copy(wt.at[i, taken, :], wt.at[i, taken, :], w_s, w_r, o).wait_send()
        share(o).wait_send()
        x_copy(lpart.at[i], lrecv.at[x], l_s, l_r, o).wait_send()
        x_copy(ubuf.at[x], ubuf.at[x], u_s, u_r, o).wait_send()
    for o in range(1, NY):
        remote(zbuf.at[z], zbuf.at[z], z_s.at[o], z_r.at[o], me).wait_send()
        remote(ybuf.at[y], ybuf.at[y], y_s.at[o], y_r.at[o], me).wait_send()
    for k in range(DOCS):
        for n in range(len(SPREAD)):
            spread(k, n).wait_send()
        for move in first_sends(k) + relay_sends(k):
            move.wait_send()

        def drain(n):
            size = pl.ds(0, n * PIECE)
            remote(fin.at[k, size, :], fin.at[k, size, :], f_s.at[k], f_r.at[k], me).wait_send()
            for e in range(2):
                remote(hid.at[k, size, :], hid.at[k, size, :], s1_s.at[k, e], s1_r.at[k, e], me).wait_send()

        pl.when(diagonal)(functools.partial(drain, NY - 1))
        pl.when(jnp.logical_not(diagonal))(functools.partial(drain, NY))


def on_device(hidden_states, head_weight, owner_pos, token_ids, teacher_margin):
    scale = float(teacher_margin.shape[0] * NC)
    dma = pltpu.SemaphoreType.DMA
    hbm = pl.BlockSpec(memory_space=pltpu.HBM)

    def stay(a):
        return pltpu.with_memory_space_constraint(a, pltpu.HBM)

    scratch = [
        pltpu.VMEM((DOCS, TERMS), jnp.int32),
        pltpu.VMEM((DOCS, 128), jnp.int32),
        pltpu.VMEM((NX, TERMS, FEATS), BF16),
        pltpu.VMEM((NX, FEATS, TERMS), BF16),
        pltpu.VMEM((NX, DOCS, TERMS), jnp.int32),
        pltpu.VMEM((DOCS, NY, 128, FEATS), BF16),
        pltpu.VMEM((HI * FEATS, LO), BF16),
        pltpu.VMEM((DOCS, NX, FEATS, TERMS), BF16),
        pltpu.VMEM((NX, DOCS, WIDE), F32),
        pltpu.VMEM((NX, DOCS, WIDE), F32),
        pltpu.VMEM((NZ, DOCS, WIDE), F32),
        pltpu.VMEM((NX, DOCS + 1, WIDE), F32),
        pltpu.VMEM((NY, 8, 128), F32),
        pltpu.VMEM((LO, HI * FEATS), F32),
        pltpu.VMEM((DOCS, NY, 128, FEATS), BF16),
        pltpu.VMEM((DOCS, 3, 128, FEATS), BF16),
        pltpu.VMEM((DOCS, 2, 128, FEATS), BF16),
        pltpu.VMEM((DOCS, 4, 128, FEATS), BF16),
        pltpu.VMEM((NX, WIDE, FEATS), BF16),
        pltpu.VMEM((NX, WIDE // 2, FEATS), BF16),
        pltpu.VMEM((NX, WIDE // 2, FEATS), BF16),
        pltpu.VMEM((2, 8, 128), F32),
        pltpu.VMEM((DOCS, 128, FEATS), BF16),
        dma((NX,)), dma((NX,)),
        dma((NX,)), dma((NX,)),
        dma((DOCS, 2)), dma((DOCS, 2)),
        dma((DOCS, 6)), dma((DOCS, 6)),
        dma((NX,)), dma((NX,)),
        dma((NZ,)), dma((NZ,)),
        dma((NX,)), dma((NX,)),
        dma((NY,)), dma((NY,)),
        dma((DOCS, 7)), dma((DOCS, 7)),
        dma((2,)), dma((2,)),
        dma((NX,)), dma((NX,)),
        dma((NX,)), dma((NX,)),
        dma((DOCS,)), dma((DOCS,)),
        dma((NX,)), dma((NX,)),
        dma((4,)),
    ]
    grad_head, grad_hidden = pl.pallas_call(
        functools.partial(kernel, scale),
        out_shape=(
            jax.ShapeDtypeStruct((WIDE, head_weight.shape[0]), BF16),
            jax.ShapeDtypeStruct(hidden_states.shape, BF16),
        ),
        in_specs=[hbm, hbm, hbm, hbm, pl.BlockSpec(memory_space=pltpu.SMEM)],
        out_specs=(pl.BlockSpec(memory_space=pl.ANY), pl.BlockSpec(memory_space=pl.ANY)),
        scratch_shapes=scratch,
        compiler_params=pltpu.CompilerParams(
            collective_id=0, has_side_effects=True, vmem_limit_bytes=VMEM_LIMIT
        ),
    )(stay(hidden_states), stay(head_weight.T), stay(owner_pos), stay(token_ids), teacher_margin)
    return grad_head[:TERMS].astype(F32).T, grad_hidden


def solution(mesh):
    return jax.shard_map(
        on_device,
        mesh=mesh,
        in_specs=(
            P("dp", "seq", "vocab"),
            P("seq", "vocab"),
            P("dp", "vocab"),
            P("dp", "seq"),
            P("dp"),
        ),
        out_specs=(P("seq", "vocab"), P("dp", "seq", "vocab")),
        check_vma=False,
    )
```

```python
import functools

import jax
import jax.numpy as jnp
from jax import lax
from jax.experimental import pallas as pl
from jax.experimental.pallas import tpu as pltpu
from jax.sharding import PartitionSpec as P

MESH = pl.DeviceIdType.MESH
F32 = jnp.float32
BF16 = jnp.bfloat16
NX, NY, NZ, NC = 4, 8, 8, 2
DOCS = 3
LO, HI = 256, 4
FEATS = 128
TERMS = 1000
WIDE = 1024
PIECE = 16
TAKEN = 504
VMEM_LIMIT = 32 * 1024 * 1024


def kernel(
    scale, hid, w, own_in, tok_in, teacher, gh_out, gx_out,
    own, tok, wt, wall, oall, hall, ht, rows, lpart, lrecv, zbuf, ubuf, ybuf, pacc, pk, relay_in, relay_out, precv, ghb, ghr, ghx, mbuf, fin,
    w_s, w_r, o_s, o_r, s1_s, s1_r, h_s, h_r, l_s, l_r, z_s, z_r, u_s, u_r, y_s, y_r,
    p_s, p_r, c_s, c_r, g_s, g_r, k_s, k_r, f_s, f_r, q_s, q_r, loc,
):
    c = lax.axis_index("dp")
    z = lax.axis_index("seq")
    v = lax.axis_index("vocab")
    y, x = v // NX, lax.rem(v, NX)

    def dev(cc, zz, yy, xx):
        return (cc, zz, yy * NX + xx)

    def turn(i, o, n):
        return lax.rem(i + o + n, n)

    def remote(src, dst, ss, rs, to):
        return pltpu.make_async_remote_copy(
            src_ref=src, dst_ref=dst, send_sem=ss, recv_sem=rs, device_id=to, device_id_type=MESH
        )

    me = dev(c, z, y, x)
    diagonal = y == z
    lane_block = pl.ds(pl.multiple_of(x * FEATS, FEATS), FEATS)

    def piece(i):
        return pl.ds(pl.multiple_of(PIECE * i, PIECE), PIECE)

    def x_copy(src, dst, ss, rs, o):
        to = dev(c, z, y, turn(x, o, NX))
        return remote(src, dst, ss.at[o], rs.at[NX - o], to)

    def y_dev(o):
        return dev(c, z, turn(y, o, NY), x)

    def scatter(k, e, o):
        j = turn(y, o, NY)
        b = turn(j, 4 * e, NY)
        src, dst = hid.at[k, piece(b), :], hall.at[k, b, piece(z), :]

        def send():
            remote(src, dst, s1_s.at[k, e], s1_r.at[k, e], dev(c, y, j, x)).start()

        if o:
            send()
        else:
            pl.when(jnp.logical_not(diagonal))(send)

            @pl.when(diagonal)
            def _():
                pltpu.make_async_copy(src, dst, s1_r.at[k, e]).start()

    SPREAD = [(1, 0), (-1, 0), (1, 1), (-1, 1), (2, 0), (-2, 0)]

    def spread(k, n):
        o, e = SPREAD[n]
        block = hall.at[k, turn(y, 4 * e, NY)]
        return remote(block, block, h_s.at[k, n], h_r.at[k, n], y_dev(o))

    def send_home(k, o):
        zz = turn(z, o, NZ)
        src, dst = fin.at[k, piece(zz), :], gx_out.at[k, piece(y), :]

        def send():
            remote(src, dst, f_s.at[k], f_r.at[k], dev(c, zz, z, x)).start()

        if o:
            send()
        else:
            pl.when(jnp.logical_not(diagonal))(send)

            @pl.when(diagonal)
            def _():
                pltpu.make_async_copy(src, dst, f_r.at[k]).start()

    taken = pl.ds(pl.multiple_of(c * (TERMS - TAKEN), 8), TAKEN)
    given = pl.ds(pl.multiple_of(c * TAKEN, 8), TERMS - TAKEN)
    lacked = pl.ds(pl.multiple_of((1 - c) * TAKEN, 8), TERMS - TAKEN)

    def share(o):
        block = wt.at[turn(x, o, NX), given, :]
        return remote(block, block, q_s.at[o], q_r.at[o], dev(1 - c, z, y, x))

    barrier = pltpu.get_barrier_semaphore()

    def greet(to):
        pl.semaphore_signal(barrier, inc=1, device_id=to, device_id_type=MESH)

    own_load = pltpu.make_async_copy(own_in, own, loc.at[2])
    own_load.start()
    tok_load = pltpu.make_async_copy(tok_in, tok, loc.at[3])
    tok_load.start()
    own_head = pltpu.make_async_copy(w.at[:, lane_block], wt.at[x], loc.at[0])
    own_head.start()
    for o in range(NY):
        greet(dev(c, y, turn(y, o, NY), x))
        greet(dev(c, turn(z, o, NZ), z, x))
    for o in range(1, NY):
        greet(dev(c, z, turn(y, o, NY), x))
        greet(dev(c, turn(z, o, NZ), y, x))
    for o in range(1, NX):
        greet(dev(c, z, y, turn(x, o, NX)))
    greet(dev(1 - c, z, y, x))

    lpart[...] = jnp.zeros_like(lpart)
    ghb[...] = jnp.zeros_like(ghb)
    own_load.wait()
    tok_load.wait()
    oall[x] = own[...]
    count = jnp.sum((tok[...] != 0).astype(F32), axis=1, keepdims=True)
    pl.semaphore_wait(barrier, 2 * NY + 2 * (NY - 1) + (NX - 1) + 1)

    for k in range(DOCS):
        for o in range(NY):
            for e in range(2):
                scatter(k, e, o)
    for o in range(1, NX):
        x_copy(own, oall.at[x], o_s, o_r, o).start()
    for o in range(1, NX):
        i = turn(x, o, NX)
        src = w.at[taken, pl.ds(pl.multiple_of(i * FEATS, FEATS), FEATS)]
        x_copy(src, wt.at[x, taken, :], w_s, w_r, o).start()

    for k in range(DOCS):
        for e in range(2):
            block = hall.at[k, turn(y, 4 * e, NY)]
            pltpu.make_async_copy(block, block, s1_r.at[k, e]).wait()
        for n in range(len(SPREAD)):
            spread(k, n).start()

    def split(owner):
        low = ((owner >> 4) & 1) * 128 + (owner >> 7) * PIECE + (owner & (PIECE - 1))
        return low, (owner >> 5) & 3

    for o in (1, 3, 2):
        i = turn(x, o, NX)
        remote(own, oall.at[i], o_s.at[o], o_r.at[o], me).wait_recv()

    for k in range(DOCS):
        for n in range(len(SPREAD)):
            o, e = SPREAD[n]
            block = hall.at[k, turn(y, 4 * e - o, NY)]
            remote(block, block, h_s.at[k, n], h_r.at[k, n], me).wait_recv()
        for j in range(NY):
            h, half = j // 2, j % 2
            ht[h * FEATS:(h + 1) * FEATS, half * 128:(half + 1) * 128] = hall[k, j].T

        def pick(i, _):
            low, high = split(oall[i, k:k + 1, :])
            tokens = lax.broadcasted_iota(jnp.int32, (LO, TERMS), 0)
            chosen = jnp.where(tokens == low, 1.0, 0.0).astype(BF16)
            four = jnp.dot(ht[...], chosen, preferred_element_type=F32)
            a, b, e, d = (four[h * FEATS:(h + 1) * FEATS] for h in range(HI))
            one = jnp.where(high < 2, jnp.where(high == 0, a, b), jnp.where(high == 2, e, d))
            rows[k, i] = one.astype(BF16)
            return 0

        lax.fori_loop(0, NX, pick, 0)

        if k == 0:
            for o in (1, 3, 2):
                i = turn(x, o, NX)
                remote(wt.at[i, taken, :], wt.at[i, taken, :], w_s.at[o], w_r.at[o], me).wait_recv()
                share(o).start()

    own_head.wait()
    for o in (1, 3, 2):
        i = turn(x, o, NX)
        remote(wt.at[i, lacked, :], wt.at[i, lacked, :], q_s.at[o], q_r.at[o], me).wait_recv()

    def dots(i, _):
        block = wt[i].T
        wall[i] = block
        head = block.astype(F32)
        for k in range(DOCS):
            lpart[i, k:k + 1, 0:TERMS] = jnp.sum(rows[k, i].astype(F32) * head, axis=0, keepdims=True)
        return 0

    lax.fori_loop(0, NX, dots, 0)

    for o in range(1, NX):
        x_copy(lpart.at[turn(x, o, NX)], lrecv.at[x], l_s, l_r, o).start()
    lrecv[x] = lpart[x]
    for o in range(1, NX):
        i = turn(x, o, NX)
        remote(lpart.at[i], lrecv.at[i], l_s.at[o], l_r.at[o], me).wait_recv()
    total = lrecv[0] + lrecv[1] + lrecv[2] + lrecv[3]
    lane = lax.broadcasted_iota(jnp.int32, (DOCS, WIDE), 1)
    zbuf[z] = jnp.where(lane < TERMS, total, count)
    for o in range(1, NZ):
        mine = zbuf.at[z]
        remote(mine, mine, z_s.at[o], z_r.at[NZ - o], dev(c, turn(z, o, NZ), y, x)).start()
    for o in range(1, NZ):
        theirs = zbuf.at[turn(z, o, NZ)]
        remote(theirs, theirs, z_s.at[o], z_r.at[o], me).wait_recv()
    total = zbuf[0]
    for i in range(1, NZ):
        total = total + zbuf[i]
    length = jnp.sum(jnp.where(lane == TERMS, total, 0.0), axis=1, keepdims=True)
    logits = total[:, 0:TERMS]
    validity = jnp.where(own[...].astype(F32) < length, 1.0, 0.0)
    soft = jnp.maximum(logits, 0.0) + jnp.log1p(jnp.exp(-jnp.abs(logits)))
    pooled = validity * jnp.log1p(soft)
    slopes = validity * jax.nn.sigmoid(logits) / (1.0 + soft)
    query, gap = pooled[0:1], pooled[1:2] - pooled[2:3]
    ubuf[x, 0:1, 0:TERMS] = (gap * slopes[0:1]).astype(BF16).astype(F32)
    ubuf[x, 1:2, 0:TERMS] = (query * slopes[1:2]).astype(BF16).astype(F32)
    ubuf[x, 2:3, 0:TERMS] = (-query * slopes[2:3]).astype(BF16).astype(F32)
    score = jnp.sum(query * gap, axis=1, keepdims=True)
    ubuf[x, 3:4, :] = jnp.broadcast_to(score, (1, WIDE))
    for o in range(1, NX):
        x_copy(ubuf.at[x], ubuf.at[x], u_s, u_r, o).start()
    for o in range(1, NX):
        i = turn(x, o, NX)
        remote(ubuf.at[i], ubuf.at[i], u_s.at[o], u_r.at[o], me).wait_recv()
    part = ubuf[0, 3:4, 0:128] + ubuf[1, 3:4, 0:128] + ubuf[2, 3:4, 0:128] + ubuf[3, 3:4, 0:128]
    ybuf[y] = jnp.broadcast_to(part, (8, 128))
    for o in range(1, NY):
        mine = ybuf.at[y]
        remote(mine, mine, y_s.at[o], y_r.at[NY - o], y_dev(o)).start()

    def far_side(k):
        return 1 if k % 2 == 0 else -1

    def first_sends(k):
        f = far_side(k)
        return [
            remote(pk.at[k, turn(y, -3, NY)], relay_in.at[k, 0], p_s.at[k, 0], p_r.at[k, 0], y_dev(-1)),
            remote(pk.at[k, turn(y, 3, NY)], relay_in.at[k, 1], p_s.at[k, 1], p_r.at[k, 1], y_dev(1)),
            remote(pk.at[k, turn(y, 4, NY)], relay_in.at[k, 2], p_s.at[k, 2], p_r.at[k, 2], y_dev(-2 * f)),
            remote(pk.at[k, turn(y, -1, NY)], precv.at[k, 0], p_s.at[k, 3], p_r.at[k, 3], y_dev(-1)),
            remote(pk.at[k, turn(y, 1, NY)], precv.at[k, 1], p_s.at[k, 4], p_r.at[k, 4], y_dev(1)),
        ]

    def relay_sends(k):
        return [
            remote(relay_out.at[k, 0], precv.at[k, 2], p_s.at[k, 5], p_r.at[k, 5], y_dev(-2)),
            remote(relay_out.at[k, 1], precv.at[k, 3], p_s.at[k, 6], p_r.at[k, 6], y_dev(2)),
        ]

    def block_terms(k):
        pacc[...] = jnp.zeros_like(pacc)

        def place(i, _):
            low, high = split(oall[i, k:k + 1, :])
            tokens = lax.broadcasted_iota(jnp.int32, (LO, TERMS), 0)
            spread_out = jnp.where(tokens == low, ubuf[i, k:k + 1, 0:TERMS], 0.0).astype(BF16)
            head = wall[i].astype(F32)
            cut = jnp.concatenate([jnp.where(high == h, head, 0.0).astype(BF16) for h in range(HI)], axis=0)
            pacc[...] += lax.dot_general(spread_out, cut, (((1,), (1,)), ((), ())), preferred_element_type=F32)
            return 0

        lax.fori_loop(0, NX, place, 0)
        for j in range(NY):
            h, half = j // 2, j % 2
            pk[k, j] = pacc[half * 128:(half + 1) * 128, h * FEATS:(h + 1) * FEATS].astype(BF16)
        for move in first_sends(k):
            move.start()

    def relay(k):
        for n in range(3):
            remote(relay_in.at[k, n], relay_in.at[k, n], p_s.at[k, n], p_r.at[k, n], me).wait_recv()
        far = relay_in[k, 2].astype(F32)
        for n, o in ((0, -2), (1, 2)):
            total = pk[k, turn(y, o, NY)].astype(F32) + relay_in[k, n].astype(F32)
            if (far_side(k) == 1) == (n == 0):
                total = total + far
            relay_out[k, n] = total.astype(BF16)
        for move in relay_sends(k):
            move.start()

    def gather_home(k):
        for n in range(4):
            remote(precv.at[k, n], precv.at[k, n], p_s.at[k, 3 + n], p_r.at[k, 3 + n], me).wait_recv()
        total = pk[k, y].astype(F32)
        for n in range(4):
            total = total + precv[k, n].astype(F32)
        fin[k] = (total * margin).astype(BF16)
        for o in range(NZ):
            send_home(k, o)

    block_terms(0)

    def head_part(i, _):
        a = ubuf[i, 0:1, 0:TERMS] * rows[0, i].astype(F32)
        b = ubuf[i, 1:2, 0:TERMS] * rows[1, i].astype(F32)
        d = ubuf[i, 2:3, 0:TERMS] * rows[2, i].astype(F32)
        ghb[i, 0:TERMS, :] = (a + b + d).astype(BF16).T
        return 0

    half = WIDE // 2
    mine_half = pl.ds(pl.multiple_of(c * half, half), half)
    other_half = pl.ds(pl.multiple_of((1 - c) * half, half), half)
    swap = remote(ghb.at[:, other_half, :], ghr, c_s.at[0], c_r.at[0], dev(1 - c, z, y, x))

    def start_heads():
        lax.fori_loop(0, NX, head_part, 0)
        swap.start()

    pl.when(c == 1)(start_heads)

    block_terms(1)
    relay(0)
    block_terms(2)

    pl.when(c == 0)(start_heads)
    for o in range(1, NY):
        theirs = ybuf.at[turn(y, o, NY)]
        remote(theirs, theirs, y_s.at[o], y_r.at[o], me).wait_recv()
    score = ybuf[0, 0:1, :]
    for i in range(1, NY):
        score = score + ybuf[i, 0:1, :]
    scaled = (score - teacher[0]) / scale
    margin = scaled[:, 0:1]
    mbuf[0] = jnp.broadcast_to(scaled, (8, 128))
    tell = remote(mbuf.at[0], mbuf.at[1], c_s.at[1], c_r.at[1], dev(1 - c, z, y, x))
    tell.start()

    def head_copy(o):
        return x_copy(ghx.at[turn(x, o, NX)], gh_out.at[mine_half, lane_block], g_s, g_r, o)

    own_out = remote(ghx.at[x], gh_out.at[mine_half, lane_block], k_s.at[0], k_r.at[0], dev(1 - c, z, y, x))
    own_move = pltpu.make_async_copy(ghx.at[x], gh_out.at[mine_half, lane_block], loc.at[1])

    def finish_heads():
        swap.wait_recv()
        tell.wait_recv()
        other_margin = mbuf[1, 0:1, 0:1]

        def head_sum(i, _):
            total = ghb[i, mine_half, :].astype(F32) * margin + ghr[i].astype(F32) * other_margin
            ghx[i] = total.astype(BF16)
            return 0

        lax.fori_loop(0, NX, head_sum, 0)
        for o in (2, 1, 3):
            head_copy(o).start()
        own_out.start()
        own_move.start()

    pl.when(c == 0)(finish_heads)
    relay(1)
    gather_home(0)
    relay(2)
    gather_home(1)
    def forward(o):
        i = turn(x, o, NX)
        block = gh_out.at[mine_half, pl.ds(pl.multiple_of(i * FEATS, FEATS), FEATS)]
        return remote(block, block, k_s.at[o], k_r.at[o], dev(1 - c, z, y, x))

    gather_home(2)
    pl.when(c == 1)(finish_heads)

    for o in (1, 3, 2):
        head_copy(o).wait_send()
        i = turn(x, o, NX)
        block = gh_out.at[mine_half, pl.ds(pl.multiple_of(i * FEATS, FEATS), FEATS)]
        remote(ghx.at[0], block, g_s.at[o], g_r.at[o], me).wait_recv()
        forward(o).start()

    for k in range(DOCS):
        pltpu.make_async_copy(fin.at[k], gx_out.at[k], f_r.at[k]).wait()
    for o in range(NX):
        i = turn(x, o, NX)
        block = gh_out.at[other_half, pl.ds(pl.multiple_of(i * FEATS, FEATS), FEATS)]
        remote(ghx.at[0], block, k_s.at[o], k_r.at[o], me).wait()
    swap.wait_send()
    tell.wait_send()
    own_move.wait()
    for o in range(1, NX):
        i = turn(x, o, NX)
        x_copy(own, oall.at[x], o_s, o_r, o).wait_send()
        x_copy(wt.at[i, taken, :], wt.at[i, taken, :], w_s, w_r, o).wait_send()
        share(o).wait_send()
        x_copy(lpart.at[i], lrecv.at[x], l_s, l_r, o).wait_send()
        x_copy(ubuf.at[x], ubuf.at[x], u_s, u_r, o).wait_send()
    for o in range(1, NY):
        remote(zbuf.at[z], zbuf.at[z], z_s.at[o], z_r.at[o], me).wait_send()
        remote(ybuf.at[y], ybuf.at[y], y_s.at[o], y_r.at[o], me).wait_send()
    for k in range(DOCS):
        for n in range(len(SPREAD)):
            spread(k, n).wait_send()
        for move in first_sends(k) + relay_sends(k):
            move.wait_send()

        def drain(n):
            size = pl.ds(0, n * PIECE)
            remote(fin.at[k, size, :], fin.at[k, size, :], f_s.at[k], f_r.at[k], me).wait_send()
            for e in range(2):
                remote(hid.at[k, size, :], hid.at[k, size, :], s1_s.at[k, e], s1_r.at[k, e], me).wait_send()

        pl.when(diagonal)(functools.partial(drain, NY - 1))
        pl.when(jnp.logical_not(diagonal))(functools.partial(drain, NY))


def on_device(hidden_states, head_weight, owner_pos, token_ids, teacher_margin):
    scale = float(teacher_margin.shape[0] * NC)
    dma = pltpu.SemaphoreType.DMA
    hbm = pl.BlockSpec(memory_space=pltpu.HBM)

    def stay(a):
        return pltpu.with_memory_space_constraint(a, pltpu.HBM)

    scratch = [
        pltpu.VMEM((DOCS, TERMS), jnp.int32),
        pltpu.VMEM((DOCS, 128), jnp.int32),
        pltpu.VMEM((NX, TERMS, FEATS), BF16),
        pltpu.VMEM((NX, FEATS, TERMS), BF16),
        pltpu.VMEM((NX, DOCS, TERMS), jnp.int32),
        pltpu.VMEM((DOCS, NY, 128, FEATS), BF16),
        pltpu.VMEM((HI * FEATS, LO), BF16),
        pltpu.VMEM((DOCS, NX, FEATS, TERMS), BF16),
        pltpu.VMEM((NX, DOCS, WIDE), F32),
        pltpu.VMEM((NX, DOCS, WIDE), F32),
        pltpu.VMEM((NZ, DOCS, WIDE), F32),
        pltpu.VMEM((NX, DOCS + 1, WIDE), F32),
        pltpu.VMEM((NY, 8, 128), F32),
        pltpu.VMEM((LO, HI * FEATS), F32),
        pltpu.VMEM((DOCS, NY, 128, FEATS), BF16),
        pltpu.VMEM((DOCS, 3, 128, FEATS), BF16),
        pltpu.VMEM((DOCS, 2, 128, FEATS), BF16),
        pltpu.VMEM((DOCS, 4, 128, FEATS), BF16),
        pltpu.VMEM((NX, WIDE, FEATS), BF16),
        pltpu.VMEM((NX, WIDE // 2, FEATS), BF16),
        pltpu.VMEM((NX, WIDE // 2, FEATS), BF16),
        pltpu.VMEM((2, 8, 128), F32),
        pltpu.VMEM((DOCS, 128, FEATS), BF16),
        dma((NX,)), dma((NX,)),
        dma((NX,)), dma((NX,)),
        dma((DOCS, 2)), dma((DOCS, 2)),
        dma((DOCS, 6)), dma((DOCS, 6)),
        dma((NX,)), dma((NX,)),
        dma((NZ,)), dma((NZ,)),
        dma((NX,)), dma((NX,)),
        dma((NY,)), dma((NY,)),
        dma((DOCS, 7)), dma((DOCS, 7)),
        dma((2,)), dma((2,)),
        dma((NX,)), dma((NX,)),
        dma((NX,)), dma((NX,)),
        dma((DOCS,)), dma((DOCS,)),
        dma((NX,)), dma((NX,)),
        dma((4,)),
    ]
    grad_head, grad_hidden = pl.pallas_call(
        functools.partial(kernel, scale),
        out_shape=(
            jax.ShapeDtypeStruct((WIDE, head_weight.shape[0]), BF16),
            jax.ShapeDtypeStruct(hidden_states.shape, BF16),
        ),
        in_specs=[hbm, hbm, hbm, hbm, pl.BlockSpec(memory_space=pltpu.SMEM)],
        out_specs=(pl.BlockSpec(memory_space=pl.ANY), pl.BlockSpec(memory_space=pl.ANY)),
        scratch_shapes=scratch,
        compiler_params=pltpu.CompilerParams(
            collective_id=0, has_side_effects=True, vmem_limit_bytes=VMEM_LIMIT
        ),
    )(stay(hidden_states), stay(head_weight.T), stay(owner_pos), stay(token_ids), teacher_margin)
    return grad_head[:TERMS].astype(F32).T, grad_hidden


def solution(mesh):
    return jax.shard_map(
        on_device,
        mesh=mesh,
        in_specs=(
            P("dp", "seq", "vocab"),
            P("seq", "vocab"),
            P("dp", "vocab"),
            P("dp", "seq"),
            P("dp"),
        ),
        out_specs=(P("seq", "vocab"), P("dp", "seq", "vocab")),
        check_vma=False,
    )
```
